32 devices in a mesh: pts: 8 (over z, x), grp: 4 (over y, core).
Axes of the slice: x: 2, y: 2, z: 4, core: 2. Of those that a mesh axis runs over, the one named last changes fastest.
Arguments:
- embeddings: bfloat16 [131072, 1024], P(('pts', 'grp')), as said below
- best_start: float32 [131072], P(('pts', 'grp')), may hold values from 0 to 2
- bounds_start: float32 [131072], P(('pts', 'grp')), may hold values from 0 to 4
- proposals: int32 [8, 32], replicated, may hold values from 0 to 131071
Outputs:
- gain_table: float32 [8, 32], replicated
- coverage: float32 [8], replicated
- best_final: float32 [131072], P(('pts', 'grp'))
- bounds_final: float32 [131072], P(('pts', 'grp'))
The draws below stay inside these ranges and needn't reach their ends.
Inputs may be any that keep to these rules, and one draw needn't show every extreme that they name: Rows are real valued embeddings of varying norm.
All inputs are finite; a program needn't handle non-finite values.
Results may differ from the reference program's by a relative error of at most 0.0003.
Values may be sent and summed in bfloat16 or wider, within the bound.
A program may use at most 64 MiB of HBM per device.

```python
import jax
import jax.numpy as jnp
from jax import lax

D = 1024
PROPS = 32
STEPS = 8
POINTS = 131072


def draw_embeddings(key, part):
    key_norm, key_scale = jax.random.split(key, 2)
    position = jnp.arange(POINTS, dtype=jnp.float32) / POINTS
    log_scale = jnp.log(3.0) * position + jax.random.uniform(key_scale, (POINTS,), jnp.float32, -0.6, 0.6)
    values = jax.random.normal(key_norm, (POINTS, D), jnp.float32)
    scaled = jnp.exp(log_scale)[:, None] * values * (0.5 * D ** (-0.25))
    return scaled.astype(jnp.bfloat16)


def plant(array, own_key, smallest, top_value):
    longest = array.shape.index(max(array.shape))
    spots = []
    for shift in (0, 1):
        where = [jax.random.randint(jax.random.fold_in(own_key, axis), (), 0, length) for axis, length in enumerate(array.shape)]
        where[longest] = (where[longest] + shift) % array.shape[longest]
        spots.append(tuple(where))
    return array.at[spots[0]].set(smallest).at[spots[1]].set(top_value)


def steps_of(key, shape, cuts, smallest, largest):
    loudness, own = 1.0, jax.random.fold_in(key, 6)
    for dim, parts in cuts:
        heights = jnp.exp(jax.random.uniform(jax.random.fold_in(own, dim), (parts,), jnp.float32, smallest / len(cuts), largest / len(cuts)))
        loudness = loudness * jnp.repeat(heights, shape[dim] // parts).reshape([-1 if axis == dim else 1 for axis in range(len(shape))])
    return loudness


def setup_inputs(seed: int = 0) -> dict:
    streams_of = jax.random.split(jax.random.key(seed), 5)
    embeddings = draw_embeddings(jax.random.fold_in(streams_of[4], 71), 0)
    best_start = jnp.clip(2.0 * jax.random.uniform(streams_of[1], (POINTS,), jnp.float32) ** steps_of(streams_of[1], (POINTS,), ((0, 32),), -0.2, 0.2), 0.0, 2.0)
    bounds_start = jnp.clip(4.0 * jax.random.uniform(streams_of[2], (POINTS,), jnp.float32) ** steps_of(streams_of[2], (POINTS,), ((0, 32),), -0.2, 0.2), 0.0, 4.0)
    proposals = plant(jax.random.randint(streams_of[3], (STEPS, PROPS), 0, POINTS), jax.random.fold_in(streams_of[3], 1), 0, POINTS - 1).astype(jnp.int32)
    return {"embeddings": embeddings, "best_start": best_start, "bounds_start": bounds_start, "proposals": proposals}


def reference(embeddings, best_start, bounds_start, proposals):
    best_sim = best_start
    bounds = bounds_start
    gain_rows = []
    cover_rows = []
    for step_index in range(STEPS):
        chosen = proposals[step_index]
        fetched = jnp.take(embeddings, chosen, axis=0)
        similarity = jnp.dot(embeddings, fetched.T, preferred_element_type=jnp.float32)
        clipped = jnp.maximum(similarity - best_sim[:, None], 0.0)
        gain_values = jnp.sum(clipped, axis=0) / POINTS
        weights = (gain_values + 0.01) / (jnp.sum(gain_values) + 0.01 * PROPS)
        mixed = jnp.dot(similarity, weights, precision=lax.Precision.HIGHEST)
        best_sim = jnp.maximum(best_sim, mixed)
        cover_rows.append(jnp.sum(best_sim) / POINTS)
        bounds = bounds.at[chosen].set(gain_values)
        gain_rows.append(gain_values)
    return jnp.stack(gain_rows), jnp.stack(cover_rows), best_sim, bounds
```

```python
import functools

import jax
import jax.numpy as jnp
from jax import lax
from jax.experimental import pallas as pl
from jax.experimental.pallas import tpu as pltpu
from jax.sharding import PartitionSpec as P

LANES = 128
SUBLANES = 8
LOAD_CHUNKS = 8
MESH = pl.DeviceIdType.MESH


def greedy_kernel(
    pts, grp, steps, props, rows, width,
    emb_hbm, best_in, bounds_in, props_in,
    gain_out, cover_out, best_out, bounds_out,
    emb, load_sem, chosen, picked, arrived, block_sum, fetched, sims, gain_src, gain_buf,
    cover_part, gain_col,
    rs_send, rs_recv, ag_send, ag_recv, gain_send, gain_recv,
):
    n = pts * grp
    blocks = (props // SUBLANES) * (width // LANES)
    spread = n // blocks
    across = width // LANES
    point_total = rows * n
    me = lax.axis_index("pts") * grp + lax.axis_index("grp")
    first_row = me * rows
    my_block = me if spread == 1 else me // spread
    is_owner = None if spread == 1 else lax.rem(me, spread) == 0

    def coords(device):
        return (device // grp, lax.rem(device, grp))

    chunk = rows // LOAD_CHUNKS
    loads = [
        pltpu.make_async_copy(
            emb_hbm.at[pl.ds(i * chunk, chunk)], emb.at[pl.ds(i * chunk, chunk)], load_sem.at[i]
        )
        for i in range(LOAD_CHUNKS)
    ]
    for load in loads:
        load.start()

    barrier = pltpu.get_barrier_semaphore()

    @pl.loop(1, n)
    def _(hop):
        pl.semaphore_signal(
            barrier, inc=1, device_id=coords(lax.rem(me + hop, n)), device_id_type=MESH
        )

    eye = lax.broadcasted_iota(jnp.int32, (props, LANES), 0) == lax.broadcasted_iota(
        jnp.int32, (props, LANES), 1
    )
    small_eye = lax.broadcasted_iota(jnp.int32, (props, props), 0) == lax.broadcasted_iota(
        jnp.int32, (props, props), 1
    )
    lane = lax.broadcasted_iota(jnp.int32, (1, LANES), 1)
    for s in range(steps):
        offsets = (props_in[pl.ds(s, 1), :] - first_row).astype(jnp.float32)
        column = jnp.sum(jnp.where(small_eye, offsets, 0.0), axis=1, keepdims=True)
        chosen[s] = jnp.broadcast_to(column, (props, LANES)).astype(jnp.int32)

    best_out[...] = best_in[...]
    bounds_out[...] = bounds_in[...]
    cover_part[...] = jnp.zeros_like(cover_part)

    def pick(low, high):
        ids = lax.broadcasted_iota(jnp.int32, (props, rows), 1)
        hot = [
            jnp.where(ids == chosen[s][:, :1], 1.0, 0.0).astype(jnp.bfloat16)
            for s in range(low, high)
        ]
        hot = jnp.concatenate(hot, axis=0)
        for c in range(width // (2 * LANES)):
            part = jnp.dot(
                hot,
                emb[:, c * 2 * LANES : (c + 1) * 2 * LANES],
                preferred_element_type=jnp.float32,
            )
            for s in range(low, high):
                for r in range(props // SUBLANES):
                    for h in range(2):
                        top = (s - low) * props + r * SUBLANES
                        picked[s, r * across + 2 * c + h] = part[
                            top : top + SUBLANES, h * LANES : (h + 1) * LANES
                        ].astype(jnp.bfloat16)

    def scatter(s):
        def to(block, device):
            hop = lax.rem(device - me + n, n)
            pltpu.make_async_remote_copy(
                src_ref=picked.at[s, block],
                dst_ref=arrived.at[s, hop - 1],
                send_sem=rs_send.at[s],
                recv_sem=rs_recv.at[s],
                device_id=coords(device),
                device_id_type=MESH,
            ).start()

        if spread == 1:

            @pl.loop(1, n)
            def _(hop):
                device = lax.rem(me + hop, n)
                to(device, device)
        else:

            @pl.loop(0, blocks)
            def _(block):
                @pl.when(block * spread != me)
                def _():
                    to(block, block * spread)

    def wait_for(ref, sem):
        pltpu.make_async_copy(ref, ref, sem).wait()

    def when_owner(f):
        if spread == 1:
            f()
        else:
            pl.when(is_owner)(f)

    def gather(s):
        @when_owner
        def _():
            wait_for(arrived.at[s], rs_recv.at[s])
            total = jnp.sum(arrived[s].astype(jnp.float32), axis=0)
            total = (total + picked[s, my_block].astype(jnp.float32)).astype(jnp.bfloat16)
            block_sum[s] = total
            fetched[s, my_block] = total

            @pl.loop(1, n)
            def _(hop):
                pltpu.make_async_remote_copy(
                    src_ref=block_sum.at[s],
                    dst_ref=fetched.at[s, my_block],
                    send_sem=ag_send.at[s],
                    recv_sem=ag_recv.at[s],
                    device_id=coords(lax.rem(me + hop, n)),
                    device_id_type=MESH,
                ).start()

    def similarity(s):
        if spread == 1:
            wait_for(fetched.at[s, pl.ds(0, blocks - 1)], ag_recv.at[s])
        else:

            @pl.when(is_owner)
            def _():
                wait_for(fetched.at[s, pl.ds(0, blocks - 1)], ag_recv.at[s])

            @pl.when(jnp.logical_not(is_owner))
            def _():
                wait_for(fetched.at[s], ag_recv.at[s])

        lines = []
        for r in range(props // SUBLANES):
            lines.append(
                jnp.concatenate(
                    [fetched[s, r * across + c].astype(jnp.float32) for c in range(across)], axis=1
                )
            )
        wanted = jnp.concatenate(lines, axis=0).astype(jnp.bfloat16)
        slot = lax.rem(s, 2)
        piece = 512
        for i in range(rows // piece):
            sims[slot, :, i * piece : (i + 1) * piece] = lax.dot_general(
                wanted,
                emb[i * piece : (i + 1) * piece, :],
                (((1,), (1,)), ((), ())),
                preferred_element_type=jnp.float32,
            )

    def send_sums(s, row):
        gain_src[s] = row
        gain_buf[s, me] = row

        @pl.loop(1, n)
        def _(hop):
            pltpu.make_async_remote_copy(
                src_ref=gain_src.at[s],
                dst_ref=gain_buf.at[s, me],
                send_sem=gain_send.at[s],
                recv_sem=gain_recv.at[s],
                device_id=coords(lax.rem(me + hop, n)),
                device_id_type=MESH,
            ).start()

    def take_sums(s):
        wait_for(gain_buf.at[s, pl.ds(0, n - 1)], gain_recv.at[s])
        return jnp.sum(gain_buf[s], axis=0) / point_total

    def refresh(s):
        gains = gain_col[...]
        ours = chosen[s]
        for i in range(rows // LANES):
            at = slice(i * LANES, (i + 1) * LANES)
            match = ours == lax.broadcasted_iota(jnp.int32, (props, LANES), 1) + i * LANES
            value = jnp.max(jnp.where(match, gains, -1.0), axis=0, keepdims=True)
            bounds_out[:, at] = jnp.where(value >= 0.0, value, bounds_out[:, at])

    def keep_cover(s, means):
        value = jnp.sum(jnp.where(lane == props, means, 0.0), axis=1, keepdims=True)
        cover_out[...] = jnp.where(lane[:, :steps] == s, value, cover_out[...])

    cover_out[...] = jnp.zeros_like(cover_out)
    early = min(2, steps)
    for load in loads:
        load.wait()
    pick(0, early)
    pl.semaphore_wait(barrier, n - 1)
    for s in range(early):
        scatter(s)
    pick(early, steps)
    for s in range(early):
        gather(s)
    scatter(early)
    similarity(0)

    @pl.loop(0, steps)
    def _(s):
        slot = lax.rem(s, 2)
        clipped = jnp.zeros((props, LANES), jnp.float32)
        for i in range(rows // LANES):
            at = slice(i * LANES, (i + 1) * LANES)
            clipped += jnp.maximum(sims[slot, :, at] - best_out[:, at], 0.0)
        column = jnp.sum(clipped, axis=1, keepdims=True)
        row = jnp.sum(jnp.where(eye, column, 0.0), axis=0, keepdims=True)
        cover = jnp.sum(cover_part[...], axis=1, keepdims=True)
        send_sums(s, jnp.where(lane == props, cover, row))

        @pl.when(s + 2 < steps)
        def _():
            gather(s + 2)

        @pl.when(s + 3 < steps)
        def _():
            scatter(s + 3)

        @pl.when(s > 0)
        def _():
            refresh(s - 1)

        @pl.when(s + 1 < steps)
        def _():
            similarity(s + 1)

        means = take_sums(s)
        gains = jnp.sum(jnp.where(eye, means, 0.0), axis=1, keepdims=True)
        weights = (gains + 0.01) / (jnp.sum(gains, axis=0, keepdims=True) + 0.01 * props)
        weights = jnp.broadcast_to(weights, (props, LANES))
        covered = jnp.zeros((1, LANES), jnp.float32)
        for i in range(rows // LANES):
            at = slice(i * LANES, (i + 1) * LANES)
            mixed = jnp.sum(sims[slot, :, at] * weights, axis=0, keepdims=True)
            best = jnp.maximum(best_out[:, at], mixed)
            best_out[:, at] = best
            covered += best
        cover_part[...] = covered
        gain_col[...] = jnp.broadcast_to(gains, (props, LANES))
        gain_out[pl.ds(s, 1), :] = means[:, :props]

        @pl.when(s > 0)
        def _():
            keep_cover(s - 1, means)

    cover = jnp.sum(cover_part[...], axis=1, keepdims=True)
    send_sums(steps, jnp.where(lane == props, cover, 0.0))
    refresh(steps - 1)
    keep_cover(steps - 1, take_sums(steps))

    @pl.loop(0, steps)
    def _(s):
        if spread == 1:
            wait_for(picked.at[s, pl.ds(0, blocks - 1)], rs_send.at[s])
            wait_for(arrived.at[s], ag_send.at[s])
        else:

            @pl.when(is_owner)
            def _():
                wait_for(picked.at[s, pl.ds(0, blocks - 1)], rs_send.at[s])
                wait_for(arrived.at[s], ag_send.at[s])

            @pl.when(jnp.logical_not(is_owner))
            def _():
                wait_for(picked.at[s], rs_send.at[s])

    @pl.loop(0, steps + 1)
    def _(s):
        wait_for(gain_buf.at[s, pl.ds(0, n - 1)], gain_send.at[s])


def on_device(pts, grp, embeddings, best_start, bounds_start, proposals):
    rows, width = embeddings.shape
    steps, props = proposals.shape
    n = pts * grp
    blocks = (props // SUBLANES) * (width // LANES)
    vmem = pl.BlockSpec(memory_space=pltpu.VMEM)
    dma = pltpu.SemaphoreType.DMA
    f32, bf16 = jnp.float32, jnp.bfloat16
    gains, cover, best, bounds = pl.pallas_call(
        functools.partial(greedy_kernel, pts, grp, steps, props, rows, width),
        out_shape=(
            jax.ShapeDtypeStruct((steps, props), f32),
            jax.ShapeDtypeStruct((1, steps), f32),
            jax.ShapeDtypeStruct((1, rows), f32),
            jax.ShapeDtypeStruct((1, rows), f32),
        ),
        in_specs=[pl.BlockSpec(memory_space=pl.ANY), vmem, vmem, vmem],
        out_specs=(vmem, vmem, vmem, vmem),
        scratch_shapes=[
            pltpu.VMEM((rows, width), bf16),
            dma((LOAD_CHUNKS,)),
            pltpu.VMEM((steps, props, LANES), jnp.int32),
            pltpu.VMEM((steps, blocks, SUBLANES, LANES), bf16),
            pltpu.VMEM((steps, n - 1, SUBLANES, LANES), bf16),
            pltpu.VMEM((steps, SUBLANES, LANES), bf16),
            pltpu.VMEM((steps, blocks, SUBLANES, LANES), bf16),
            pltpu.VMEM((2, props, rows), f32),
            pltpu.VMEM((steps + 1, 1, LANES), f32),
            pltpu.VMEM((steps + 1, n, 1, LANES), f32),
            pltpu.VMEM((1, LANES), f32),
            pltpu.VMEM((props, LANES), f32),
            dma((steps,)),
            dma((steps,)),
            dma((steps,)),
            dma((steps,)),
            dma((steps + 1,)),
            dma((steps + 1,)),
        ],
        compiler_params=pltpu.CompilerParams(
            collective_id=0, has_side_effects=True, vmem_limit_bytes=56 * 1024 * 1024
        ),
    )(embeddings, best_start.reshape(1, rows), bounds_start.reshape(1, rows), proposals)
    return gains, cover.reshape(steps), best.reshape(rows), bounds.reshape(rows)


def solution(mesh):
    placed = (P(("pts", "grp"), None), P(("pts", "grp")), P(("pts", "grp")), P())
    return jax.shard_map(
        functools.partial(on_device, mesh.shape["pts"], mesh.shape["grp"]),
        mesh=mesh,
        in_specs=placed,
        out_specs=(P(), P(), P(("pts", "grp")), P(("pts", "grp"))),
        check_vma=False,
    )
```

```python
import functools

import jax
import jax.numpy as jnp
from jax import lax
from jax.experimental import pallas as pl
from jax.experimental.pallas import tpu as pltpu
from jax.sharding import PartitionSpec as P

LANES = 128
SUBLANES = 8
LOAD_CHUNKS = 8
UNROLLED_PEERS = 32
MESH = pl.DeviceIdType.MESH


def greedy_kernel(
    pts, grp, steps, props, rows, width,
    emb_hbm, best_in, bounds_in, props_in,
    gain_out, cover_out, best_out, bounds_out,
    emb, load_sem, chosen, picked, arrived, block_sum, fetched, sims, gain_src, gain_buf,
    gain_col, found,
    rs_send, rs_recv, ag_send, ag_recv, gain_send, gain_recv,
):
    n = pts * grp
    blocks = (props // SUBLANES) * (width // LANES)
    spread = n // blocks
    across = width // LANES
    point_total = rows * n
    me = lax.axis_index("pts") * grp + lax.axis_index("grp")
    first_row = me * rows
    my_block = me if spread == 1 else me // spread
    is_owner = None if spread == 1 else lax.rem(me, spread) == 0

    my_pts, my_grp = lax.axis_index("pts"), lax.axis_index("grp")

    def flip(position, size, step):
        if size & (size - 1):
            return lax.rem(position + step, size)
        for bit in [1 << k for k in range(size.bit_length()) if step >> k & 1]:
            position = position + bit - 2 * bit * lax.rem(position // bit, 2)
        return position

    grp_at = [flip(my_grp, grp, step) for step in range(grp)]

    def coords(device):
        return (device // grp, lax.rem(device, grp))

    def each_peer(f):
        def line(at, step, skip):
            for turn in range(grp - 1, skip - 1, -1):
                f((at, grp_at[turn]), step * grp + turn - 1)

        if n <= UNROLLED_PEERS:
            for step in range(pts - 1, 0, -1):
                line(pts_at[step], step, 0)
        else:
            pl.loop(1, pts)(lambda step: line(lax.rem(my_pts + step, pts), step, 0))
        line(my_pts, 0, 1)

    if n <= UNROLLED_PEERS:
        pts_at = [flip(my_pts, pts, step) for step in range(pts)]

    chunk = rows // LOAD_CHUNKS
    loads = [
        pltpu.make_async_copy(
            emb_hbm.at[pl.ds(i * chunk, chunk)], emb.at[pl.ds(i * chunk, chunk)], load_sem.at[i]
        )
        for i in range(LOAD_CHUNKS)
    ]
    for load in loads:
        load.start()

    barrier = pltpu.get_barrier_semaphore()

    each_peer(
        lambda peer, _: pl.semaphore_signal(barrier, inc=1, device_id=peer, device_id_type=MESH)
    )

    eye = lax.broadcasted_iota(jnp.int32, (props, LANES), 0) == lax.broadcasted_iota(
        jnp.int32, (props, LANES), 1
    )
    small_eye = lax.broadcasted_iota(jnp.int32, (props, props), 0) == lax.broadcasted_iota(
        jnp.int32, (props, props), 1
    )
    lane = lax.broadcasted_iota(jnp.int32, (1, LANES), 1)
    for s in range(steps):
        offsets = (props_in[pl.ds(s, 1), :] - first_row).astype(jnp.float32)
        column = jnp.sum(jnp.where(small_eye, offsets, 0.0), axis=1, keepdims=True)
        chosen[s] = jnp.broadcast_to(column, (props, LANES)).astype(jnp.int32)

    best_out[...] = best_in[...]
    bounds_out[...] = bounds_in[...]

    def pick(low, high, loads=()):
        wide = 2 * LANES
        stop = (high - low) * props
        cuts = len(loads) or 1
        part = rows // cuts
        for i in range(cuts):
            if loads:
                loads[i].wait()
            ids = lax.broadcasted_iota(jnp.int32, (props, part), 1) + i * part
            hot = [
                jnp.where(ids == chosen[s][:, :1], 1.0, 0.0).astype(jnp.bfloat16)
                for s in range(low, high)
            ]
            hot = jnp.concatenate(hot, axis=0)
            for c in range(width // wide):
                at = slice(c * wide, (c + 1) * wide)
                term = jnp.dot(
                    hot, emb[i * part : (i + 1) * part, at], preferred_element_type=jnp.float32
                )
                found[:stop, at] = term if i == 0 else found[:stop, at] + term
        for s in range(low, high):
            for r in range(props // SUBLANES):
                top = (s - low) * props + r * SUBLANES
                for c in range(across):
                    picked[s, r * across + c] = found[
                        top : top + SUBLANES, c * LANES : (c + 1) * LANES
                    ].astype(jnp.bfloat16)

    def scatter(s):
        def to(block, peer, slot):
            pltpu.make_async_remote_copy(
                src_ref=picked.at[s, block],
                dst_ref=arrived.at[s, slot],
                send_sem=rs_send.at[s],
                recv_sem=rs_recv.at[s],
                device_id=peer,
                device_id_type=MESH,
            ).start()

        if spread == 1:
            each_peer(lambda peer, slot: to(peer[0] * grp + peer[1], peer, slot))
        else:

            @pl.loop(0, blocks)
            def _(block):
                @pl.when(block * spread != me)
                def _():
                    device = block * spread
                    at, turn = coords(device)
                    step = lax.rem(at - my_pts + pts, pts)
                    to(block, (at, turn), step * grp + lax.rem(turn - my_grp + grp, grp) - 1)

    def wait_for(ref, sem):
        pltpu.make_async_copy(ref, ref, sem).wait()

    def when_owner(f):
        if spread == 1:
            f()
        else:
            pl.when(is_owner)(f)

    def gather(s):
        @when_owner
        def _():
            wait_for(arrived.at[s], rs_recv.at[s])
            total = jnp.sum(arrived[s].astype(jnp.float32), axis=0)
            total = (total + picked[s, my_block].astype(jnp.float32)).astype(jnp.bfloat16)
            block_sum[s] = total
            fetched[s, my_block] = total

            each_peer(
                lambda peer, _: pltpu.make_async_remote_copy(
                    src_ref=block_sum.at[s],
                    dst_ref=fetched.at[s, my_block],
                    send_sem=ag_send.at[s],
                    recv_sem=ag_recv.at[s],
                    device_id=peer,
                    device_id_type=MESH,
                ).start()
            )

    def similarity(s):
        if spread == 1:
            wait_for(fetched.at[s, pl.ds(0, blocks - 1)], ag_recv.at[s])
        else:

            @pl.when(is_owner)
            def _():
                wait_for(fetched.at[s, pl.ds(0, blocks - 1)], ag_recv.at[s])

            @pl.when(jnp.logical_not(is_owner))
            def _():
                wait_for(fetched.at[s], ag_recv.at[s])

        lines = []
        for r in range(props // SUBLANES):
            lines.append(
                jnp.concatenate(
                    [fetched[s, r * across + c].astype(jnp.float32) for c in range(across)], axis=1
                )
            )
        wanted = jnp.concatenate(lines, axis=0).astype(jnp.bfloat16)
        slot = lax.rem(s, 2)
        piece = 512
        for i in range(rows // piece):
            sims[slot, :, i * piece : (i + 1) * piece] = lax.dot_general(
                wanted,
                emb[i * piece : (i + 1) * piece, :],
                (((1,), (1,)), ((), ())),
                preferred_element_type=jnp.float32,
            )

    def send_sums(s, row):
        gain_src[s] = row
        gain_buf[s, me] = row

        each_peer(
            lambda peer, _: pltpu.make_async_remote_copy(
                src_ref=gain_src.at[s],
                dst_ref=gain_buf.at[s, me],
                send_sem=gain_send.at[s],
                recv_sem=gain_recv.at[s],
                device_id=peer,
                device_id_type=MESH,
            ).start()
        )

    def take_sums(s):
        wait_for(gain_buf.at[s, pl.ds(0, n - 1)], gain_recv.at[s])
        return jnp.sum(gain_buf[s], axis=0) / point_total

    def refresh(s):
        gains = gain_col[...]
        ours = chosen[s]
        for i in range(rows // LANES):
            at = slice(i * LANES, (i + 1) * LANES)
            match = ours == lax.broadcasted_iota(jnp.int32, (props, LANES), 1) + i * LANES
            value = jnp.max(jnp.where(match, gains, -1.0), axis=0, keepdims=True)
            bounds_out[:, at] = jnp.where(value >= 0.0, value, bounds_out[:, at])

    def keep_cover(s, means):
        value = jnp.sum(jnp.where(lane == props, means, 0.0), axis=1, keepdims=True)
        cover_out[...] = jnp.where(lane[:, :steps] == s, value, cover_out[...])

    cover_out[...] = jnp.zeros_like(cover_out)
    early = min(2, steps)
    pick(0, early, loads)
    pl.semaphore_wait(barrier, n - 1)
    for s in range(early):
        scatter(s)
    if early < steps:
        pick(early, steps)
    for s in range(early):
        gather(s)
    if early < steps:
        scatter(early)
    similarity(0)

    def as_row(clipped):
        column = jnp.sum(clipped, axis=1, keepdims=True)
        return jnp.sum(jnp.where(eye, column, 0.0), axis=0, keepdims=True)

    lane_blocks = [slice(i * LANES, (i + 1) * LANES) for i in range(rows // LANES)]
    clipped = jnp.zeros((props, LANES), jnp.float32)
    for at in lane_blocks:
        clipped += jnp.maximum(sims[0, :, at] - best_out[:, at], 0.0)
    send_sums(0, as_row(clipped))
    for s in range(2, min(3, steps)):
        gather(s)
    for s in range(3, min(4, steps)):
        scatter(s)
    for s in range(1, min(2, steps)):
        similarity(s)

    @pl.loop(0, steps)
    def _(s):
        slot = lax.rem(s, 2)
        means = take_sums(s)
        gains = jnp.sum(jnp.where(eye, means, 0.0), axis=1, keepdims=True)
        weights = (gains + 0.01) / (jnp.sum(gains, axis=0, keepdims=True) + 0.01 * props)
        weights = jnp.broadcast_to(weights, (props, LANES))
        covered = jnp.zeros((1, LANES), jnp.float32)
        clipped = jnp.zeros((props, LANES), jnp.float32)
        for at in lane_blocks:
            mixed = jnp.sum(sims[slot, :, at] * weights, axis=0, keepdims=True)
            best = jnp.maximum(best_out[:, at], mixed)
            best_out[:, at] = best
            covered += best
            clipped += jnp.maximum(sims[1 - slot, :, at] - best, 0.0)
        cover = jnp.sum(covered, axis=1, keepdims=True)
        send_sums(s + 1, jnp.where(lane == props, cover, as_row(clipped)))

        @pl.when(s + 3 < steps)
        def _():
            gather(s + 3)

        @pl.when(s + 4 < steps)
        def _():
            scatter(s + 4)

        gain_col[...] = jnp.broadcast_to(gains, (props, LANES))
        gain_out[pl.ds(s, 1), :] = means[:, :props]
        refresh(s)

        @pl.when(s > 0)
        def _():
            keep_cover(s - 1, means)

        @pl.when(s + 2 < steps)
        def _():
            similarity(s + 2)

    keep_cover(steps - 1, take_sums(steps))

    @pl.loop(0, steps)
    def _(s):
        if spread == 1:
            wait_for(picked.at[s, pl.ds(0, blocks - 1)], rs_send.at[s])
            wait_for(arrived.at[s], ag_send.at[s])
        else:

            @pl.when(is_owner)
            def _():
                wait_for(picked.at[s, pl.ds(0, blocks - 1)], rs_send.at[s])
                wait_for(arrived.at[s], ag_send.at[s])

            @pl.when(jnp.logical_not(is_owner))
            def _():
                wait_for(picked.at[s], rs_send.at[s])

    @pl.loop(0, steps + 1)
    def _(s):
        wait_for(gain_buf.at[s, pl.ds(0, n - 1)], gain_send.at[s])


def hand_over(*refs):
    for source, target in zip(refs[:4], refs[4:]):
        target[...] = source[...]


def on_device(pts, grp, embeddings, best_start, bounds_start, proposals):
    rows, width = embeddings.shape
    steps, props = proposals.shape
    n = pts * grp
    blocks = (props // SUBLANES) * (width // LANES)
    vmem = pl.BlockSpec(memory_space=pltpu.VMEM)
    dma = pltpu.SemaphoreType.DMA
    f32, bf16 = jnp.float32, jnp.bfloat16
    gains, cover, best, bounds = pl.pallas_call(
        functools.partial(greedy_kernel, pts, grp, steps, props, rows, width),
        out_shape=(
            jax.ShapeDtypeStruct((steps, props), f32),
            jax.ShapeDtypeStruct((1, steps), f32),
            jax.ShapeDtypeStruct((1, rows), f32),
            jax.ShapeDtypeStruct((1, rows), f32),
        ),
        in_specs=[pl.BlockSpec(memory_space=pl.ANY), vmem, vmem, vmem],
        out_specs=(vmem, vmem, vmem, vmem),
        scratch_shapes=[
            pltpu.VMEM((rows, width), bf16),
            dma((LOAD_CHUNKS,)),
            pltpu.VMEM((steps, props, LANES), jnp.int32),
            pltpu.VMEM((steps, blocks, SUBLANES, LANES), bf16),
            pltpu.VMEM((steps, n - 1, SUBLANES, LANES), bf16),
            pltpu.VMEM((steps, SUBLANES, LANES), bf16),
            pltpu.VMEM((steps, blocks, SUBLANES, LANES), bf16),
            pltpu.VMEM((2, props, rows), f32),
            pltpu.VMEM((steps + 1, 1, LANES), f32),
            pltpu.VMEM((steps + 1, n, 1, LANES), f32),
            pltpu.VMEM((props, LANES), f32),
            pltpu.VMEM((steps * props, width), f32),
            dma((steps,)),
            dma((steps,)),
            dma((steps,)),
            dma((steps,)),
            dma((steps + 1,)),
            dma((steps + 1,)),
        ],
        compiler_params=pltpu.CompilerParams(
            collective_id=0, has_side_effects=True, vmem_limit_bytes=56 * 1024 * 1024
        ),
    )(embeddings, best_start.reshape(1, rows), bounds_start.reshape(1, rows), proposals)
    results = (gains, cover, best, bounds)
    gains, cover, best, bounds = pl.pallas_call(
        hand_over,
        out_shape=tuple(jax.ShapeDtypeStruct(x.shape, x.dtype) for x in results),
        in_specs=[vmem] * 4,
        out_specs=(vmem,) * 4,
    )(*results)
    return gains, cover.reshape(steps), best.reshape(rows), bounds.reshape(rows)


def solution(mesh):
    placed = (P(("pts", "grp"), None), P(("pts", "grp")), P(("pts", "grp")), P())
    return jax.shard_map(
        functools.partial(on_device, mesh.shape["pts"], mesh.shape["grp"]),
        mesh=mesh,
        in_specs=placed,
        out_specs=(P(), P(), P(("pts", "grp")), P(("pts", "grp"))),
        check_vma=False,
    )
```

```python
import functools

import jax
import jax.numpy as jnp
from jax import lax
from jax.experimental import pallas as pl
from jax.experimental.pallas import tpu as pltpu
from jax.sharding import PartitionSpec as P

LANES = 128
SUBLANES = 8
LOAD_CHUNKS = 8
UNROLLED_PEERS = 32
MESH = pl.DeviceIdType.MESH


def greedy_kernel(
    pts, grp, steps, props, rows, width,
    emb_hbm, best_in, bounds_in, props_in,
    gain_out, cover_out, best_out, bounds_out,
    emb, load_sem, chosen, picked, arrived, block_sum, fetched, sims, gain_src, gain_buf,
    gain_col, found,
    rs_send, rs_recv, ag_send, ag_recv, gain_send, gain_recv,
):
    n = pts * grp
    blocks = (props // SUBLANES) * (width // LANES)
    spread = n // blocks
    across = width // LANES
    point_total = rows * n
    me = lax.axis_index("pts") * grp + lax.axis_index("grp")
    first_row = me * rows
    my_block = me if spread == 1 else me // spread
    is_owner = None if spread == 1 else lax.rem(me, spread) == 0

    my_pts, my_grp = lax.axis_index("pts"), lax.axis_index("grp")

    def flip(position, size, step):
        if size & (size - 1):
            return lax.rem(position + step, size)
        for bit in [1 << k for k in range(size.bit_length()) if step >> k & 1]:
            position = position + bit - 2 * bit * lax.rem(position // bit, 2)
        return position

    grp_at = [flip(my_grp, grp, step) for step in range(grp)]

    def coords(device):
        return (device // grp, lax.rem(device, grp))

    def each_peer(f):
        def line(at, step, skip):
            for turn in range(grp - 1, skip - 1, -1):
                f((at, grp_at[turn]), step * grp + turn - 1)

        if n <= UNROLLED_PEERS:
            for step in range(pts - 1, 0, -1):
                line(pts_at[step], step, 0)
        else:
            pl.loop(1, pts)(lambda step: line(lax.rem(my_pts + step, pts), step, 0))
        line(my_pts, 0, 1)

    if n <= UNROLLED_PEERS:
        pts_at = [flip(my_pts, pts, step) for step in range(pts)]

    chunk = rows // LOAD_CHUNKS
    loads = [
        pltpu.make_async_copy(
            emb_hbm.at[pl.ds(i * chunk, chunk)], emb.at[pl.ds(i * chunk, chunk)], load_sem.at[i]
        )
        for i in range(LOAD_CHUNKS)
    ]
    for load in loads:
        load.start()

    barrier = pltpu.get_barrier_semaphore()

    each_peer(
        lambda peer, _: pl.semaphore_signal(barrier, inc=1, device_id=peer, device_id_type=MESH)
    )

    eye = lax.broadcasted_iota(jnp.int32, (props, LANES), 0) == lax.broadcasted_iota(
        jnp.int32, (props, LANES), 1
    )
    small_eye = lax.broadcasted_iota(jnp.int32, (props, props), 0) == lax.broadcasted_iota(
        jnp.int32, (props, props), 1
    )
    lane = lax.broadcasted_iota(jnp.int32, (1, LANES), 1)
    for s in range(steps):
        offsets = (props_in[pl.ds(s, 1), :] - first_row).astype(jnp.float32)
        column = jnp.sum(jnp.where(small_eye, offsets, 0.0), axis=1, keepdims=True)
        chosen[s] = jnp.broadcast_to(column, (props, LANES)).astype(jnp.int32)

    best_out[...] = best_in[...]
    bounds_out[...] = bounds_in[...]

    def pick(low, high, loads=()):
        wide = 2 * LANES
        stop = (high - low) * props
        cuts = len(loads) or 1
        part = rows // cuts
        for i in range(cuts):
            if loads:
                loads[i].wait()
            ids = lax.broadcasted_iota(jnp.int32, (props, part), 1) + i * part
            hot = [
                jnp.where(ids == chosen[s][:, :1], 1.0, 0.0).astype(jnp.bfloat16)
                for s in range(low, high)
            ]
            hot = jnp.concatenate(hot, axis=0)
            for c in range(width // wide):
                at = slice(c * wide, (c + 1) * wide)
                term = jnp.dot(
                    hot, emb[i * part : (i + 1) * part, at], preferred_element_type=jnp.float32
                )
                found[:stop, at] = term if i == 0 else found[:stop, at] + term
        for s in range(low, high):
            for r in range(props // SUBLANES):
                top = (s - low) * props + r * SUBLANES
                for c in range(across):
                    picked[s, r * across + c] = found[
                        top : top + SUBLANES, c * LANES : (c + 1) * LANES
                    ].astype(jnp.bfloat16)

    def scatter(s):
        def to(block, peer, slot):
            pltpu.make_async_remote_copy(
                src_ref=picked.at[s, block],
                dst_ref=arrived.at[s, slot],
                send_sem=rs_send.at[s],
                recv_sem=rs_recv.at[s],
                device_id=peer,
                device_id_type=MESH,
            ).start()

        if spread == 1:
            each_peer(lambda peer, slot: to(peer[0] * grp + peer[1], peer, slot))
        else:

            @pl.loop(0, blocks)
            def _(block):
                @pl.when(block * spread != me)
                def _():
                    device = block * spread
                    at, turn = coords(device)
                    step = lax.rem(at - my_pts + pts, pts)
                    to(block, (at, turn), step * grp + lax.rem(turn - my_grp + grp, grp) - 1)

    def wait_for(ref, sem):
        pltpu.make_async_copy(ref, ref, sem).wait()

    def when_owner(f):
        if spread == 1:
            f()
        else:
            pl.when(is_owner)(f)

    def gather(s):
        @when_owner
        def _():
            wait_for(arrived.at[s], rs_recv.at[s])
            total = jnp.sum(arrived[s].astype(jnp.float32), axis=0)
            total = (total + picked[s, my_block].astype(jnp.float32)).astype(jnp.bfloat16)
            block_sum[s] = total
            fetched[s, my_block] = total

            each_peer(
                lambda peer, _: pltpu.make_async_remote_copy(
                    src_ref=block_sum.at[s],
                    dst_ref=fetched.at[s, my_block],
                    send_sem=ag_send.at[s],
                    recv_sem=ag_recv.at[s],
                    device_id=peer,
                    device_id_type=MESH,
                ).start()
            )

    def similarity(s):
        if spread == 1:
            wait_for(fetched.at[s, pl.ds(0, blocks - 1)], ag_recv.at[s])
        else:

            @pl.when(is_owner)
            def _():
                wait_for(fetched.at[s, pl.ds(0, blocks - 1)], ag_recv.at[s])

            @pl.when(jnp.logical_not(is_owner))
            def _():
                wait_for(fetched.at[s], ag_recv.at[s])

        lines = []
        for r in range(props // SUBLANES):
            lines.append(
                jnp.concatenate(
                    [fetched[s, r * across + c].astype(jnp.float32) for c in range(across)], axis=1
                )
            )
        wanted = jnp.concatenate(lines, axis=0).astype(jnp.bfloat16)
        slot = lax.rem(s, 2)
        piece = 512
        for i in range(rows // piece):
            sims[slot, :, i * piece : (i + 1) * piece] = lax.dot_general(
                wanted,
                emb[i * piece : (i + 1) * piece, :],
                (((1,), (1,)), ((), ())),
                preferred_element_type=jnp.float32,
            )

    def send_sums(s, row):
        gain_src[s] = row
        gain_buf[s, me] = row

        each_peer(
            lambda peer, _: pltpu.make_async_remote_copy(
                src_ref=gain_src.at[s],
                dst_ref=gain_buf.at[s, me],
                send_sem=gain_send.at[s],
                recv_sem=gain_recv.at[s],
                device_id=peer,
                device_id_type=MESH,
            ).start()
        )

    def take_sums(s):
        wait_for(gain_buf.at[s, pl.ds(0, n - 1)], gain_recv.at[s])
        return jnp.sum(gain_buf[s], axis=0) / point_total

    def refresh(s):
        gains = gain_col[...]
        ours = chosen[s]
        for i in range(rows // LANES):
            at = slice(i * LANES, (i + 1) * LANES)
            match = ours == lax.broadcasted_iota(jnp.int32, (props, LANES), 1) + i * LANES
            value = jnp.max(jnp.where(match, gains, -1.0), axis=0, keepdims=True)
            bounds_out[:, at] = jnp.where(value >= 0.0, value, bounds_out[:, at])

    def keep_cover(s, means):
        value = jnp.sum(jnp.where(lane == props, means, 0.0), axis=1, keepdims=True)
        cover_out[...] = jnp.where(lane[:, :steps] == s, value, cover_out[...])

    cover_out[...] = jnp.zeros_like(cover_out)
    early = min(2, steps)
    pick(0, early, loads)
    pl.semaphore_wait(barrier, n - 1)
    for s in range(early):
        scatter(s)
    if early < steps:
        pick(early, steps)
    for s in range(early):
        gather(s)
    for s in range(early, min(early + 2, steps)):
        scatter(s)
    similarity(0)

    def as_row(clipped):
        column = jnp.sum(clipped, axis=1, keepdims=True)
        return jnp.sum(jnp.where(eye, column, 0.0), axis=0, keepdims=True)

    lane_blocks = [slice(i * LANES, (i + 1) * LANES) for i in range(rows // LANES)]
    clipped = jnp.zeros((props, LANES), jnp.float32)
    for at in lane_blocks:
        clipped += jnp.maximum(sims[0, :, at] - best_out[:, at], 0.0)
    send_sums(0, as_row(clipped))
    for s in range(2, min(3, steps)):
        gather(s)
    for s in range(4, min(5, steps)):
        scatter(s)
    for s in range(1, min(2, steps)):
        similarity(s)

    @pl.loop(0, steps)
    def _(s):
        slot = lax.rem(s, 2)
        means = take_sums(s)
        gains = jnp.sum(jnp.where(eye, means, 0.0), axis=1, keepdims=True)
        weights = (gains + 0.01) / (jnp.sum(gains, axis=0, keepdims=True) + 0.01 * props)
        weights = jnp.broadcast_to(weights, (props, LANES))
        covered = jnp.zeros((1, LANES), jnp.float32)
        clipped = jnp.zeros((props, LANES), jnp.float32)
        for at in lane_blocks:
            mixed = jnp.sum(sims[slot, :, at] * weights, axis=0, keepdims=True)
            best = jnp.maximum(best_out[:, at], mixed)
            best_out[:, at] = best
            covered += best
            clipped += jnp.maximum(sims[1 - slot, :, at] - best, 0.0)
        cover = jnp.sum(covered, axis=1, keepdims=True)
        send_sums(s + 1, jnp.where(lane == props, cover, as_row(clipped)))

        @pl.when(s + 3 < steps)
        def _():
            gather(s + 3)

        @pl.when(s + 5 < steps)
        def _():
            scatter(s + 5)

        gain_col[...] = jnp.broadcast_to(gains, (props, LANES))
        gain_out[pl.ds(s, 1), :] = means[:, :props]
        refresh(s)

        @pl.when(s > 0)
        def _():
            keep_cover(s - 1, means)

        @pl.when(s + 2 < steps)
        def _():
            similarity(s + 2)

    keep_cover(steps - 1, take_sums(steps))

    @pl.loop(0, steps)
    def _(s):
        if spread == 1:
            wait_for(picked.at[s, pl.ds(0, blocks - 1)], rs_send.at[s])
            wait_for(arrived.at[s], ag_send.at[s])
        else:

            @pl.when(is_owner)
            def _():
                wait_for(picked.at[s, pl.ds(0, blocks - 1)], rs_send.at[s])
                wait_for(arrived.at[s], ag_send.at[s])

            @pl.when(jnp.logical_not(is_owner))
            def _():
                wait_for(picked.at[s], rs_send.at[s])

    @pl.loop(0, steps + 1)
    def _(s):
        wait_for(gain_buf.at[s, pl.ds(0, n - 1)], gain_send.at[s])


def hand_over(*refs):
    for source, target in zip(refs[:4], refs[4:]):
        target[...] = source[...]


def on_device(pts, grp, embeddings, best_start, bounds_start, proposals):
    rows, width = embeddings.shape
    steps, props = proposals.shape
    n = pts * grp
    blocks = (props // SUBLANES) * (width // LANES)
    vmem = pl.BlockSpec(memory_space=pltpu.VMEM)
    dma = pltpu.SemaphoreType.DMA
    f32, bf16 = jnp.float32, jnp.bfloat16
    gains, cover, best, bounds = pl.pallas_call(
        functools.partial(greedy_kernel, pts, grp, steps, props, rows, width),
        out_shape=(
            jax.ShapeDtypeStruct((steps, props), f32),
            jax.ShapeDtypeStruct((1, steps), f32),
            jax.ShapeDtypeStruct((1, rows), f32),
            jax.ShapeDtypeStruct((1, rows), f32),
        ),
        in_specs=[pl.BlockSpec(memory_space=pl.ANY), vmem, vmem, vmem],
        out_specs=(vmem, vmem, vmem, vmem),
        scratch_shapes=[
            pltpu.VMEM((rows, width), bf16),
            dma((LOAD_CHUNKS,)),
            pltpu.VMEM((steps, props, LANES), jnp.int32),
            pltpu.VMEM((steps, blocks, SUBLANES, LANES), bf16),
            pltpu.VMEM((steps, n - 1, SUBLANES, LANES), bf16),
            pltpu.VMEM((steps, SUBLANES, LANES), bf16),
            pltpu.VMEM((steps, blocks, SUBLANES, LANES), bf16),
            pltpu.VMEM((2, props, rows), f32),
            pltpu.VMEM((steps + 1, 1, LANES), f32),
            pltpu.VMEM((steps + 1, n, 1, LANES), f32),
            pltpu.VMEM((props, LANES), f32),
            pltpu.VMEM((steps * props, width), f32),
            dma((steps,)),
            dma((steps,)),
            dma((steps,)),
            dma((steps,)),
            dma((steps + 1,)),
            dma((steps + 1,)),
        ],
        compiler_params=pltpu.CompilerParams(
            collective_id=0, has_side_effects=True, vmem_limit_bytes=56 * 1024 * 1024
        ),
    )(embeddings, best_start.reshape(1, rows), bounds_start.reshape(1, rows), proposals)
    results = (gains, cover, best, bounds)
    gains, cover, best, bounds = pl.pallas_call(
        hand_over,
        out_shape=tuple(jax.ShapeDtypeStruct(x.shape, x.dtype) for x in results),
        in_specs=[vmem] * 4,
        out_specs=(vmem,) * 4,
    )(*results)
    return gains, cover.reshape(steps), best.reshape(rows), bounds.reshape(rows)


def solution(mesh):
    placed = (P(("pts", "grp"), None), P(("pts", "grp")), P(("pts", "grp")), P())
    return jax.shard_map(
        functools.partial(on_device, mesh.shape["pts"], mesh.shape["grp"]),
        mesh=mesh,
        in_specs=placed,
        out_specs=(P(), P(), P(("pts", "grp")), P(("pts", "grp"))),
        check_vma=False,
    )
```
